1024 devices in a mesh: dp: 16 (over x, core), group: 64 (over z, y).
Axes of the slice: x: 8, y: 8, z: 8, core: 2. Of those that a mesh axis runs over, the one named last changes fastest.
Arguments:
- acts: bfloat16 [2048, 16384], P('dp', 'group'), may hold values from -6 to 6
- cotan: bfloat16 [2048, 8192], P('dp'), may hold values from -0.1875 to 0.1875
- stats: float32 [16, 64, 512, 512], P('dp', 'group'), as said below
- roots: bfloat16 [16, 64, 512, 512], P('dp', 'group'), as said below
- owner: int32 [64], replicated, may hold values from 0 to 63, as said below
- task_of: int32 [64], replicated, may hold values from 0 to 63, as said below
- counts: int32 [64], replicated, may hold values from 1 to 2
Outputs:
- update: bfloat16 [8192, 16384], P('dp', 'group')
- new_stats: float32 [16, 64, 512, 512], P('dp', 'group')
- new_roots: bfloat16 [16, 64, 512, 512], P('dp', 'group')
The draws below stay inside these ranges and needn't reach their ends.
Inputs may be any that keep to these rules, and one draw needn't show every extreme that they name: A permutation; owner[t] is the group index of the device that keeps task t's statistic; task t is the left (t even) or right (t odd) factor of the block whose columns are held by group indices t - t % 2 and t - t % 2 + 1. `task_of`: the inverse permutation of owner. Each stats[k, o] is symmetric positive definite. Each roots[k, t] is symmetric.
All inputs are finite; a program needn't handle non-finite values.
Results may differ from the reference program's by a relative error of at most 0.0055.
The reference program's roundings to bfloat16 on the way (of `gradient`, `factor` and `left_part`) count: a program that leaves them out, or rounds other values in their place, can miss the bound.
Values may be sent and summed in bfloat16 or wider, within the bound.
No kernel may reach another device: no remote copies, remote signals or barrier semaphores. Data moves between devices by JAX's collectives and lax.ppermute only.
A program may use at most 128 MiB of HBM per device.

```python
import jax
import jax.numpy as jnp
from jax import lax

B = 512
TOKENS = 2048
OUT = 8192
IN = 16384
N_DP = 16
N_GROUP = 64


def routing_tables(key):
    owner = jax.random.permutation(jax.random.fold_in(key, 17), N_GROUP).astype(jnp.int32)
    task_of = jnp.argsort(owner, stable=True).astype(jnp.int32)
    return (owner, task_of)


def draw_owner(key, part):
    return routing_tables(key)[0]


def draw_task_of(key, part):
    return routing_tables(key)[1]


def draw_stats(key, part):
    slots = N_DP * N_GROUP
    slot_keys = jax.random.split(jax.random.fold_in(key, 35), slots)
    ranking = jax.vmap(lambda each: jax.random.permutation(each, B))(slot_keys)
    ranking = ranking.reshape(N_DP, N_GROUP, B).astype(jnp.float32) + 1.0
    rough = jax.random.uniform(jax.random.fold_in(key, 33), (N_DP, N_GROUP, B), jnp.float32, 0.6, 1.4)
    base = jax.random.normal(jax.random.fold_in(key, 31), (N_DP, N_GROUP, B, B), jnp.float32)
    exponent = 1.3
    level = 0.05
    weights = level * B ** 1.5 * rough * ranking ** (-exponent)
    coupled = jnp.einsum('...ab,...cb->...ac', base, base) / B + 0.5 * jnp.eye(B, dtype=jnp.float32)
    scale_root = jnp.sqrt(weights)
    return scale_root[..., :, None] * coupled * scale_root[..., None, :]


def draw_roots(key, part):
    noise = jax.random.normal(jax.random.fold_in(key, 41), (N_DP, N_GROUP, B, B), jnp.float32)
    symmetric = (noise + jnp.swapaxes(noise, -1, -2)) * (0.5 / (2.0 * B) ** 0.5)
    diagonal = jax.random.uniform(jax.random.fold_in(key, 42), (N_DP, N_GROUP, B), jnp.float32, 0.5, 1.5)
    return (symmetric + diagonal[..., None] * jnp.eye(B, dtype=jnp.float32)).astype(jnp.bfloat16)


def with_ends(array, stream_key, smallest, top_value):
    extent = array.shape
    index_at = [jax.random.randint(jax.random.fold_in(stream_key, axis), (), 0, extent[axis]) for axis in range(len(extent))]
    array = array.at[tuple(index_at)].set(smallest)
    longest = extent.index(max(extent))
    index_at[longest] = (index_at[longest] + 1) % extent[longest]
    return array.at[tuple(index_at)].set(top_value)


def raised(entries, key, source, target, blocks, factor):
    def block_of(dim):
        return (jnp.arange(entries.shape[dim]) // (entries.shape[dim] // blocks)).reshape((-1,) + (1,) * (entries.ndim - 1 - dim))

    near = jax.random.permutation(key, blocks)[block_of(target)]
    far = (block_of(target) + blocks // 2) % blocks
    return jnp.where((block_of(source) == near) | (block_of(source) == far), factor * entries, entries)


def levels(key, dims, shards, low, top_value):
    def one(dim, parts):
        heights = jax.random.uniform(jax.random.fold_in(jax.random.fold_in(key, 6), dim), (parts,), jnp.float32, low / len(shards), top_value / len(shards))
        return jnp.repeat(jnp.exp(heights), dims[dim] // parts).reshape((-1,) + (1,) * (len(dims) - dim - 1))

    gain = one(*shards[0])
    for cut in shards[1:]:
        gain = gain * one(*cut)
    return gain


def centred(stream_key, shape, spread, most, cuts=(), kind=jnp.bfloat16):
    result = jax.random.normal(stream_key, shape, jnp.float32) * spread
    if len(cuts) > 0:
        result = levels(stream_key, shape, cuts, -0.22, 0.18) * result
    return jnp.clip(result, min=-most, max=most).astype(kind)


def gaussian_with(rng, shape, width, bound, cuts, heavy, held_as=jnp.bfloat16):
    values = width * jax.random.normal(rng, shape, jnp.float32)
    if cuts:
        values = values * levels(rng, shape, cuts, -0.22, 0.18)
    return jnp.clip(raised(values, jax.random.fold_in(rng, 3), *heavy), -bound, bound).astype(held_as)


def setup_inputs(seed: int = 0) -> dict:
    splits = jax.random.split(jax.random.key(seed), 8)
    acts = centred(splits[0], (TOKENS, IN), 1.0, 6.0, ((0, 16), (1, 64)))
    cotan = gaussian_with(splits[1], (TOKENS, OUT), TOKENS ** -0.5, 0.1875, ((0, 16),), (0, 1, 16, 2.0))
    stats = draw_stats(jax.random.fold_in(splits[7], 71), 0)
    roots = draw_roots(jax.random.fold_in(splits[7], 71), 0)
    owner = draw_owner(jax.random.fold_in(splits[7], 71), 0)
    task_of = draw_task_of(jax.random.fold_in(splits[7], 71), 0)
    counts = with_ends(jax.random.randint(splits[6], (N_GROUP,), 1, 3), jax.random.fold_in(splits[6], 1), 1, 2).astype(jnp.int32)
    return dict(acts=acts, cotan=cotan, stats=stats, roots=roots, owner=owner, task_of=task_of, counts=counts)


decay_rate = 0.9
ridge = 0.001
highest = lax.Precision.HIGHEST

def newton_root(statistic, turns):
    identity = jnp.eye(statistic.shape[0], dtype=jnp.float32)
    matrix = statistic + ridge * identity
    frobenius = jnp.sqrt(jnp.sum(matrix * matrix))
    initial_root = identity * frobenius ** (-0.25)
    start_scaled = matrix / frobenius

    def one_turn(index, current_state):
        root_now, scaled = current_state
        step_matrix = (5.0 * identity - scaled) / 4.0
        root_now = jnp.dot(root_now, step_matrix, precision=highest)
        squared = jnp.dot(step_matrix, step_matrix, precision=highest)
        scaled = jnp.dot(squared, jnp.dot(squared, scaled, precision=highest), precision=highest)
        return (root_now, scaled)
    return lax.fori_loop(0, turns, one_turn, (initial_root, start_scaled))[0]

def reference(acts, cotan, stats, roots, owner, task_of, counts):
    gradient = jnp.dot(cotan.T, acts, preferred_element_type=jnp.float32).astype(jnp.bfloat16)
    blocks = gradient.reshape(N_DP, B, N_GROUP // 2, B).transpose(0, 2, 1, 3)
    matched_pairs = roots.reshape(N_DP, N_GROUP // 2, 2, B, B)
    slot_counts = counts[task_of]

    def one_row(row_args):
        row_blocks, row_stats, row_roots = row_args
        left_part = jnp.einsum('jab,jbc->jac', row_roots[:, 0].astype(jnp.float32), row_blocks.astype(jnp.float32)).astype(jnp.bfloat16)
        row_update = jnp.einsum('jab,jbc->jac', left_part.astype(jnp.float32), row_roots[:, 1].astype(jnp.float32)).astype(jnp.bfloat16)
        factors = jnp.stack([row_blocks, jnp.swapaxes(row_blocks, 1, 2)], 1).reshape(N_GROUP, B, B)
        grouped_per_slot = factors[task_of].astype(jnp.float32)
        gram_product = jnp.einsum('yne,yie->yni', grouped_per_slot, grouped_per_slot)
        row_new = decay_rate * row_stats + gram_product
        slot_roots = lax.map(lambda entry: newton_root(entry[0], entry[1]), (row_new, slot_counts))
        return (row_update, row_new, slot_roots[owner].astype(jnp.bfloat16))
    updates, new_stats, new_roots = lax.map(one_row, (blocks, stats, matched_pairs))
    update = updates.transpose(0, 2, 1, 3).reshape(N_DP * B, N_GROUP // 2 * B)
    return (update, new_stats, new_roots)
```

```python
import jax
import jax.numpy as jnp
from jax import lax
from jax.experimental import pallas as pl
from jax.experimental.pallas import tpu as pltpu
from jax.sharding import PartitionSpec as P

decay_rate = 0.9
ridge = 0.001
BF = jnp.bfloat16
F32 = jnp.float32
LANES = 128
SIDE = 8
PARTS = 4
STAT_ROWS = 24
STRIP = 32


def dot(a, b, dims=((1,), (0,))):
    return lax.dot_general(a, b, (dims, ((), ())), preferred_element_type=F32)


def smem():
    return pl.BlockSpec(memory_space=pltpu.SMEM)


def vmem(count):
    return [pl.BlockSpec(memory_space=pltpu.VMEM)] * count


def strip_tiles(groups):
    half = groups // 2
    low = half * 8
    for a in range(half):
        for strip, place, row, lane in (
            (a, 0, a * 8, 0),
            (a, 1, a * 8, 1),
            (a, 2, low + a * 8, 0),
            (half + a, 0, low + a * 8, 1),
            (half + a, 1, low + a * 8, 2),
            (half + a, 2, low + a * 8, 3),
        ):
            yield strip, place * 8, row, lane * LANES


def pack_kernel(stats, acts, out):
    groups = out.shape[0]
    for strip, place, row, lane in strip_tiles(groups):
        out[strip, place : place + 8, :] = stats[row : row + 8, lane : lane + LANES].astype(BF)
    for tile in range(groups // 2):
        row, lane = tile // 2 * 8, tile % 2 * LANES
        piece = acts[row : row + 8, lane : lane + LANES]
        out[2 * tile, STAT_ROWS:, :] = piece
        out[2 * tile + 1, STAT_ROWS:, :] = piece


def select_kernel(stat_source, act_source, middle, out):
    def one(o, carry):
        out[o, :STAT_ROWS, :] = middle[stat_source[o], :STAT_ROWS, :]
        out[o, STAT_ROWS:, :] = middle[act_source[o], STAT_ROWS:, :]
        return carry

    lax.fori_loop(0, out.shape[0], one, 0, unroll=8)


def acts_kernel(scalars, own, other, arrived, out):
    cols = own.shape[1]
    half = scalars[0]

    @pl.when(half == 0)
    def _():
        out[:, :cols] = own[...]
        out[:, cols : 2 * cols] = other[...]

    @pl.when(half == 1)
    def _():
        out[:, :cols] = other[...]
        out[:, cols : 2 * cols] = own[...]

    for strip in range(arrived.shape[0]):
        tile, side = strip // 2, strip % 2
        row, lane = tile // 2 * 8, 2 * cols + side * cols + tile % 2 * LANES
        out[row : row + 8, lane : lane + LANES] = arrived[strip, STAT_ROWS:, :]


def cotan_kernel(scalars, cotan, out, buffer, sems):
    count = out.shape[0]

    def copy(k):
        start = pl.multiple_of((k * PARTS + scalars[0]) * LANES, LANES)
        return pltpu.make_async_copy(cotan.at[:, pl.ds(start, LANES)], buffer.at[k], sems.at[k])

    for k in range(count):
        copy(k).start()
    for k in range(count):
        copy(k).wait()
        out[k] = buffer[k].T


def gram_into(block, odd, out_ref):
    @pl.when(odd == 0)
    def _():
        out_ref[...] = dot(block, block, ((1,), (1,)))

    @pl.when(odd == 1)
    def _():
        out_ref[...] = dot(block, block, ((0,), (0,)))


def step_kernel(
    scalars,
    part0,
    part1,
    part2,
    part3,
    acts,
    own_root,
    other_root,
    arrived,
    stats,
    update,
    new_stats,
    new_root,
    block,
    gram,
    old,
    root,
):
    half = scalars[0]
    turns = scalars[1]
    kept_odd = scalars[2]
    first_part = scalars[3]
    n = stats.shape[0]
    half_cols = n // 2

    for shift, part in enumerate((part0, part1, part2, part3)):
        rows = jnp.concatenate([part[i] for i in range(part.shape[0])], 1)
        start = pl.multiple_of((first_part + shift) % PARTS * LANES, LANES)
        block[pl.ds(start, LANES), :] = dot(rows, acts[...]).astype(BF)

    kept = block[:, n:]
    gram_into(kept, kept_odd, gram)
    new_stats[...] = decay_rate * stats[...] + gram[...]

    own = block[:, :n]

    @pl.when(half == 0)
    def _():
        left_part = dot(own_root[...], own).astype(BF)
        update[...] = dot(left_part, other_root[:, :half_cols]).astype(BF)

    @pl.when(half == 1)
    def _():
        left_part = dot(other_root[...], own).astype(BF)
        update[...] = dot(left_part, own_root[:, half_cols:]).astype(BF)

    for strip, place, row, lane in strip_tiles(arrived.shape[0]):
        old[row : row + 8, lane : lane + LANES] = arrived[strip, place : place + 8, :].astype(F32)
    old[:half_cols, half_cols:] = old[half_cols:, :half_cols].T

    gram_into(own, half, gram)
    identity = (
        lax.broadcasted_iota(jnp.int32, (n, n), 0) == lax.broadcasted_iota(jnp.int32, (n, n), 1)
    ).astype(F32)
    matrix = decay_rate * old[...] + gram[...] + ridge * identity
    square_sum = jnp.sum(jnp.sum(matrix * matrix, axis=0, keepdims=True), axis=1, keepdims=True)
    inv_norm = lax.rsqrt(square_sum)
    scaled = matrix * inv_norm
    gram[...] = scaled
    root[...] = jnp.sqrt(jnp.sqrt(inv_norm)) * (1.25 * identity - 0.25 * scaled)

    def one_turn(_, carry):
        m = gram[...]
        mb = m.astype(BF)
        q = ((dot(mb, mb) - 10.0 * m) * 0.0625).astype(BF)
        t = 1.5625 * m + dot(q, mb)
        m = 1.5625 * t + dot(q, t.astype(BF))
        gram[...] = m
        x = root[...]
        root[...] = 1.25 * x - 0.25 * dot(x.astype(BF), m.astype(BF))
        return carry

    lax.fori_loop(1, turns, one_turn, 0)
    new_root[...] = root[...].astype(BF)


def from_partner(x, partner):
    count = lax.axis_size("group")
    return lax.ppermute(x, "group", [(partner(i), i) for i in range(count)])


def z_up(i):
    return (i + SIDE) % (SIDE * SIDE)


def z_down(i):
    return (i - SIDE) % (SIDE * SIDE)


def y_outer(i):
    y = i % SIDE
    return i - y + (y + (1 if y % 2 else -1)) % SIDE


def pair(i):
    return i ^ 1


def per_device(acts, cotan, stats, roots, owner, task_of, counts):
    groups = lax.axis_size("group")
    rows = lax.axis_size("dp")
    position = lax.axis_index("group")
    n = stats.shape[-1]
    half = position % 2
    my_task = task_of[position]
    old_stats = stats[0, 0]
    own_root = roots[0, 0]

    strips = pl.pallas_call(
        pack_kernel,
        out_shape=jax.ShapeDtypeStruct((groups, STRIP, LANES), BF),
        in_specs=vmem(2),
        out_specs=vmem(1)[0],
        name="pack_strips",
    )(old_stats, acts)
    middle = lax.all_to_all(strips, "group", split_axis=0, concat_axis=0, tiled=True)
    chosen = pl.pallas_call(
        select_kernel,
        out_shape=jax.ShapeDtypeStruct((groups, STRIP, LANES), BF),
        in_specs=[smem(), smem()] + vmem(1),
        out_specs=vmem(1)[0],
        name="select_strips",
    )(owner, task_of // 2 * 2 + half, middle)
    arrived = lax.all_to_all(chosen, "group", split_axis=0, concat_axis=0, tiled=True)

    other_acts = from_partner(acts, pair)
    both_acts = pl.pallas_call(
        acts_kernel,
        out_shape=jax.ShapeDtypeStruct((acts.shape[0], 2 * n), BF),
        in_specs=[smem()] + vmem(3),
        out_specs=vmem(1)[0],
        name="join_acts",
    )(jnp.reshape(half, (1,)), acts, other_acts, arrived)
    all_acts = lax.all_gather(both_acts, "dp", axis=0, tiled=True)

    first_part = (position // SIDE + 2 * (position % SIDE)) % PARTS
    tokens = cotan.shape[0]
    part = pl.pallas_call(
        cotan_kernel,
        out_shape=jax.ShapeDtypeStruct((rows, LANES, tokens), BF),
        in_specs=[smem(), pl.BlockSpec(memory_space=pl.ANY)],
        out_specs=vmem(1)[0],
        scratch_shapes=[pltpu.VMEM((rows, tokens, LANES), BF), pltpu.SemaphoreType.DMA((rows,))],
        name="cotan_part",
    )(jnp.reshape(first_part, (1,)), cotan)
    part0 = lax.all_to_all(part, "dp", split_axis=0, concat_axis=0, tiled=True)
    part1 = from_partner(part0, z_up)
    part2 = from_partner(part0, y_outer)
    part3 = from_partner(part0, z_down)

    other_root = from_partner(own_root, pair)

    update, new_stats, new_root = pl.pallas_call(
        step_kernel,
        out_shape=(
            jax.ShapeDtypeStruct((n, n // 2), BF),
            jax.ShapeDtypeStruct((n, n), F32),
            jax.ShapeDtypeStruct((n, n), BF),
        ),
        in_specs=[smem()] + vmem(9),
        out_specs=tuple(vmem(3)),
        scratch_shapes=[
            pltpu.VMEM((n, 2 * n), BF),
            pltpu.VMEM((n, n), F32),
            pltpu.VMEM((n, n), F32),
            pltpu.VMEM((n, n), F32),
        ],
        name="shampoo_step",
    )(
        jnp.stack([half, counts[position], my_task % 2, first_part]),
        part0,
        part1,
        part2,
        part3,
        all_acts,
        own_root,
        other_root,
        arrived,
        old_stats,
    )
    return (update, new_stats[None, None], new_root[None, None])


def solution(mesh):
    return jax.shard_map(
        per_device,
        mesh=mesh,
        in_specs=(
            P("dp", "group"),
            P("dp", None),
            P("dp", "group", None, None),
            P("dp", "group", None, None),
            P(),
            P(),
            P(),
        ),
        out_specs=(P("dp", "group"), P("dp", "group", None, None), P("dp", "group", None, None)),
        check_vma=False,
    )
```

```python
import jax
import jax.numpy as jnp
from jax import lax
from jax.experimental import pallas as pl
from jax.experimental.pallas import tpu as pltpu
from jax.sharding import PartitionSpec as P

decay_rate = 0.9
ridge = 0.001
BF = jnp.bfloat16
F32 = jnp.float32
LANES = 128
SIDE = 8
PARTS = 8
STEPS = ((1, 0), (2, 0), (0, 1), (1, 1), (0, -1), (-2, 0), (-1, 0))
STAT_ROWS = 24
STRIP = 32


def dot(a, b, dims=((1,), (0,))):
    return lax.dot_general(a, b, (dims, ((), ())), preferred_element_type=F32)


def smem():
    return pl.BlockSpec(memory_space=pltpu.SMEM)


def vmem(count):
    return [pl.BlockSpec(memory_space=pltpu.VMEM)] * count


def strip_tiles(groups):
    half = groups // 2
    low = half * 8
    for a in range(half):
        for strip, place, row, lane in (
            (a, 0, a * 8, 0),
            (a, 1, a * 8, 1),
            (a, 2, low + a * 8, 0),
            (half + a, 0, low + a * 8, 1),
            (half + a, 1, low + a * 8, 2),
            (half + a, 2, low + a * 8, 3),
        ):
            yield strip, place * 8, row, lane * LANES


def pack_kernel(stats, acts, out):
    groups = out.shape[0]
    for strip, place, row, lane in strip_tiles(groups):
        out[strip, place : place + 8, :] = stats[row : row + 8, lane : lane + LANES].astype(BF)
    for tile in range(groups // 2):
        row, lane = tile // 2 * 8, tile % 2 * LANES
        piece = acts[row : row + 8, lane : lane + LANES]
        out[2 * tile, STAT_ROWS:, :] = piece
        out[2 * tile + 1, STAT_ROWS:, :] = piece


def select_kernel(stat_source, act_source, middle, out):
    def one(o, carry):
        out[o, :STAT_ROWS, :] = middle[stat_source[o], :STAT_ROWS, :]
        out[o, STAT_ROWS:, :] = middle[act_source[o], STAT_ROWS:, :]
        return carry

    lax.fori_loop(0, out.shape[0], one, 0, unroll=8)


def acts_kernel(scalars, own, other, arrived, out):
    cols = own.shape[1]
    half = scalars[0]

    @pl.when(half == 0)
    def _():
        out[:, :cols] = own[...]
        out[:, cols : 2 * cols] = other[...]

    @pl.when(half == 1)
    def _():
        out[:, :cols] = other[...]
        out[:, cols : 2 * cols] = own[...]

    for strip in range(arrived.shape[0]):
        tile, side = strip // 2, strip % 2
        row, lane = tile // 2 * 8, 2 * cols + side * cols + tile % 2 * LANES
        out[row : row + 8, lane : lane + LANES] = arrived[strip, STAT_ROWS:, :]


def cotan_kernel(scalars, cotan, out, buffer, sems):
    count = buffer.shape[0]
    depth = out.shape[0] // count
    fold = LANES // depth
    part = scalars[0]

    def copy(k):
        start = pl.multiple_of((k * (PARTS // fold) + part // fold) * LANES, LANES)
        return pltpu.make_async_copy(cotan.at[:, pl.ds(start, LANES)], buffer.at[k], sems.at[k])

    for k in range(count):
        copy(k).start()
    for k in range(count):
        copy(k).wait()
    for side in range(fold):

        @pl.when(part % fold == side)
        def _():
            for k in range(count):
                turned = buffer[k].T
                out[k * depth : (k + 1) * depth, :] = turned[side * depth : (side + 1) * depth, :]


def gram_into(block, odd, out_ref):
    @pl.when(odd == 0)
    def _():
        out_ref[...] = dot(block, block, ((1,), (1,)))

    @pl.when(odd == 1)
    def _():
        out_ref[...] = dot(block, block, ((0,), (0,)))


def step_kernel(scalars, *refs):
    parts, refs = refs[:PARTS], refs[PARTS:]
    acts, own_root, other_root, arrived, stats, *refs = refs
    update, new_stats, new_root, cotan_t, block, gram, old, root = refs
    half = scalars[0]
    turns = scalars[1]
    kept_odd = scalars[2]
    first_part = scalars[3]
    n = stats.shape[0]
    half_cols = n // 2
    depth = n // PARTS

    for shift, part in enumerate(parts):
        start = pl.multiple_of((first_part + shift) % PARTS * depth, depth)
        for i in range(part.shape[0]):
            cotan_t[pl.ds(start, depth), i * LANES : (i + 1) * LANES] = part[i]
    block[...] = dot(cotan_t[...], acts[...]).astype(BF)

    kept = block[:, n:]
    gram_into(kept, kept_odd, gram)
    new_stats[...] = decay_rate * stats[...] + gram[...]

    own = block[:, :n]

    @pl.when(half == 0)
    def _():
        left_part = dot(own_root[...], own).astype(BF)
        update[...] = dot(left_part, other_root[:, :half_cols]).astype(BF)

    @pl.when(half == 1)
    def _():
        left_part = dot(other_root[...], own).astype(BF)
        update[...] = dot(left_part, own_root[:, half_cols:]).astype(BF)

    for strip, place, row, lane in strip_tiles(arrived.shape[0]):
        old[row : row + 8, lane : lane + LANES] = arrived[strip, place : place + 8, :].astype(F32)
    old[:half_cols, half_cols:] = old[half_cols:, :half_cols].T

    gram_into(own, half, gram)
    identity = (
        lax.broadcasted_iota(jnp.int32, (n, n), 0) == lax.broadcasted_iota(jnp.int32, (n, n), 1)
    ).astype(F32)
    matrix = decay_rate * old[...] + gram[...] + ridge * identity
    square_sum = jnp.sum(jnp.sum(matrix * matrix, axis=0, keepdims=True), axis=1, keepdims=True)
    inv_norm = lax.rsqrt(square_sum)
    scaled = matrix * inv_norm
    gram[...] = scaled
    root[...] = jnp.sqrt(jnp.sqrt(inv_norm)) * (1.25 * identity - 0.25 * scaled)

    def one_turn(_, carry):
        m = gram[...]
        mb = m.astype(BF)
        q = ((dot(mb, mb) - 10.0 * m) * 0.0625).astype(BF)
        t = 1.5625 * m + dot(q, mb)
        m = 1.5625 * t + dot(q, t.astype(BF))
        gram[...] = m
        x = root[...]
        root[...] = 1.25 * x - 0.25 * dot(x.astype(BF), m.astype(BF))
        return carry

    lax.fori_loop(1, turns, one_turn, 0)
    new_root[...] = root[...].astype(BF)


def from_partner(x, partner):
    count = lax.axis_size("group")
    return lax.ppermute(x, "group", [(partner(i), i) for i in range(count)])


def stepped(i, step):
    z, y = i // SIDE, i % SIDE
    return (z + step[0]) % SIDE * SIDE + (y + step[1]) % SIDE


def pair(i):
    return i ^ 1


def per_device(acts, cotan, stats, roots, owner, task_of, counts):
    groups = lax.axis_size("group")
    rows = lax.axis_size("dp")
    position = lax.axis_index("group")
    n = stats.shape[-1]
    half = position % 2
    my_task = task_of[position]
    old_stats = stats[0, 0]
    own_root = roots[0, 0]

    strips = pl.pallas_call(
        pack_kernel,
        out_shape=jax.ShapeDtypeStruct((groups, STRIP, LANES), BF),
        in_specs=vmem(2),
        out_specs=vmem(1)[0],
        name="pack_strips",
    )(old_stats, acts)
    middle = lax.all_to_all(strips, "group", split_axis=0, concat_axis=0, tiled=True)
    chosen = pl.pallas_call(
        select_kernel,
        out_shape=jax.ShapeDtypeStruct((groups, STRIP, LANES), BF),
        in_specs=[smem(), smem()] + vmem(1),
        out_specs=vmem(1)[0],
        name="select_strips",
    )(owner, task_of // 2 * 2 + half, middle)
    arrived = lax.all_to_all(chosen, "group", split_axis=0, concat_axis=0, tiled=True)

    other_acts = from_partner(acts, pair)
    both_acts = pl.pallas_call(
        acts_kernel,
        out_shape=jax.ShapeDtypeStruct((acts.shape[0], 2 * n), BF),
        in_specs=[smem()] + vmem(3),
        out_specs=vmem(1)[0],
        name="join_acts",
    )(jnp.reshape(half, (1,)), acts, other_acts, arrived)
    all_acts = lax.all_gather(both_acts, "dp", axis=0, tiled=True)

    first_part = (position // SIDE + 3 * (position % SIDE)) % PARTS
    tokens = cotan.shape[0]
    depth = n // PARTS
    piece = pl.pallas_call(
        cotan_kernel,
        out_shape=jax.ShapeDtypeStruct((rows * depth, tokens), BF),
        in_specs=[smem(), pl.BlockSpec(memory_space=pl.ANY)],
        out_specs=vmem(1)[0],
        scratch_shapes=[pltpu.VMEM((rows, tokens, LANES), BF), pltpu.SemaphoreType.DMA((rows,))],
        name="cotan_part",
    )(jnp.reshape(first_part, (1,)), cotan)
    pieces = lax.all_gather(piece, "dp", axis=0)
    part = lax.dynamic_slice_in_dim(pieces, lax.axis_index("dp") * depth, depth, 1)
    parts = [part] + [from_partner(part, lambda i, step=step: stepped(i, step)) for step in STEPS]

    other_root = from_partner(own_root, pair)

    update, new_stats, new_root = pl.pallas_call(
        step_kernel,
        out_shape=(
            jax.ShapeDtypeStruct((n, n // 2), BF),
            jax.ShapeDtypeStruct((n, n), F32),
            jax.ShapeDtypeStruct((n, n), BF),
        ),
        in_specs=[smem()] + vmem(PARTS + 5),
        out_specs=tuple(vmem(3)),
        scratch_shapes=[
            pltpu.VMEM((n, rows * tokens), BF),
            pltpu.VMEM((n, 2 * n), BF),
            pltpu.VMEM((n, n), F32),
            pltpu.VMEM((n, n), F32),
            pltpu.VMEM((n, n), F32),
        ],
        name="shampoo_step",
    )(
        jnp.stack([half, counts[position], my_task % 2, first_part]),
        *parts,
        all_acts,
        own_root,
        other_root,
        arrived,
        old_stats,
    )
    return (update, new_stats[None, None], new_root[None, None])


def solution(mesh):
    return jax.shard_map(
        per_device,
        mesh=mesh,
        in_specs=(
            P("dp", "group"),
            P("dp", None),
            P("dp", "group", None, None),
            P("dp", "group", None, None),
            P(),
            P(),
            P(),
        ),
        out_specs=(P("dp", "group"), P("dp", "group", None, None), P("dp", "group", None, None)),
        check_vma=False,
    )
```

```python
import jax
import jax.numpy as jnp
from jax import lax
from jax.experimental import pallas as pl
from jax.experimental.pallas import tpu as pltpu
from jax.sharding import PartitionSpec as P

decay_rate = 0.9
ridge = 0.001
BF = jnp.bfloat16
F32 = jnp.float32
LANES = 128
SIDE = 8
PARTS = 8
STEPS = ((1, 0), (2, 0), (0, 1), (1, 1), (0, -1), (-2, 0), (-1, 0))
STAT_ROWS = 24
STRIP = 32


def dot(a, b, dims=((1,), (0,))):
    return lax.dot_general(a, b, (dims, ((), ())), preferred_element_type=F32)


def smem():
    return pl.BlockSpec(memory_space=pltpu.SMEM)


def vmem(count):
    return [pl.BlockSpec(memory_space=pltpu.VMEM)] * count


def strip_tiles(groups):
    half = groups // 2
    low = half * 8
    for a in range(half):
        for strip, place, row, lane in (
            (a, 0, a * 8, 0),
            (a, 1, a * 8, 1),
            (a, 2, low + a * 8, 0),
            (half + a, 0, low + a * 8, 1),
            (half + a, 1, low + a * 8, 2),
            (half + a, 2, low + a * 8, 3),
        ):
            yield strip, place * 8, row, lane * LANES


def pack_kernel(stats, acts, out):
    groups = out.shape[0]
    for strip, place, row, lane in strip_tiles(groups):
        out[strip, place : place + 8, :] = stats[row : row + 8, lane : lane + LANES].astype(BF)
    for tile in range(groups // 2):
        row, lane = tile // 2 * 8, tile % 2 * LANES
        piece = acts[row : row + 8, lane : lane + LANES]
        out[2 * tile, STAT_ROWS:, :] = piece
        out[2 * tile + 1, STAT_ROWS:, :] = piece


def select_kernel(stat_source, act_source, middle, stats_out, acts_out):
    def one(o, carry):
        stats_out[o] = middle[stat_source[o], :STAT_ROWS, :]
        acts_out[o] = middle[act_source[o], STAT_ROWS:, :]
        return carry

    lax.fori_loop(0, middle.shape[0], one, 0, unroll=8)


def acts_kernel(scalars, own, other, arrived, out):
    cols = own.shape[1]
    half = scalars[0]

    @pl.when(half == 0)
    def _():
        out[:, :cols] = own[...]
        out[:, cols : 2 * cols] = other[...]

    @pl.when(half == 1)
    def _():
        out[:, :cols] = other[...]
        out[:, cols : 2 * cols] = own[...]

    for strip in range(arrived.shape[0]):
        tile, side = strip // 2, strip % 2
        row, lane = tile // 2 * 8, 2 * cols + side * cols + tile % 2 * LANES
        out[row : row + 8, lane : lane + LANES] = arrived[strip]


def cotan_kernel(scalars, cotan, out, buffer, sems):
    count = buffer.shape[0]
    depth = out.shape[0] // count
    fold = LANES // depth
    part = scalars[0]

    def copy(k):
        start = pl.multiple_of((k * (PARTS // fold) + part // fold) * LANES, LANES)
        return pltpu.make_async_copy(cotan.at[:, pl.ds(start, LANES)], buffer.at[k], sems.at[k])

    for k in range(count):
        copy(k).start()
    for k in range(count):
        copy(k).wait()
    for side in range(fold):

        @pl.when(part % fold == side)
        def _():
            for k in range(count):
                turned = buffer[k].T
                out[k * depth : (k + 1) * depth, :] = turned[side * depth : (side + 1) * depth, :]


def gram_into(block, odd, out_ref):
    @pl.when(odd == 0)
    def _():
        out_ref[...] = dot(block, block, ((1,), (1,)))

    @pl.when(odd == 1)
    def _():
        out_ref[...] = dot(block, block, ((0,), (0,)))


def step_kernel(scalars, *refs):
    parts, refs = refs[:PARTS], refs[PARTS:]
    acts_in, own_root_in, other_root_in, arrived_in, stats_in, *refs = refs
    update, new_stats, new_root, *refs = refs
    cotan_t, acts, own_root, other_root, arrived, stats, gram, old, root, sems = refs
    half = scalars[0]
    turns = scalars[1]
    kept_odd = scalars[2]
    first_part = scalars[3]
    n = stats.shape[0]
    half_cols = n // 2
    depth = n // PARTS

    fetches = [
        pltpu.make_async_copy(source, target, sems.at[index])
        for index, (source, target) in enumerate(
            (
                (arrived_in, arrived),
                (acts_in.at[:, :n], acts.at[0]),
                (own_root_in, own_root),
                (other_root_in, other_root),
                (acts_in.at[:, n:], acts.at[1]),
                (stats_in, stats),
            )
        )
    ]
    for fetch in fetches:
        fetch.start()

    for shift, part in enumerate(parts):
        start = pl.multiple_of((first_part + shift) % PARTS * depth, depth)
        for i in range(part.shape[0]):
            cotan_t[pl.ds(start, depth), i * LANES : (i + 1) * LANES] = part[i]

    fetches[0].wait()
    for strip, place, row, lane in strip_tiles(arrived.shape[0]):
        old[row : row + 8, lane : lane + LANES] = arrived[strip, place : place + 8, :].astype(F32)
    old[:half_cols, half_cols:] = old[half_cols:, :half_cols].T

    fetches[1].wait()
    own = dot(cotan_t[...], acts[0]).astype(BF)
    fetches[2].wait()
    fetches[3].wait()

    @pl.when(half == 0)
    def _():
        left_part = dot(own_root[...], own).astype(BF)
        update[...] = dot(left_part, other_root[:, :half_cols]).astype(BF)

    @pl.when(half == 1)
    def _():
        left_part = dot(other_root[...], own).astype(BF)
        update[...] = dot(left_part, own_root[:, half_cols:]).astype(BF)

    gram_into(own, half, gram)
    identity = (
        lax.broadcasted_iota(jnp.int32, (n, n), 0) == lax.broadcasted_iota(jnp.int32, (n, n), 1)
    ).astype(F32)
    matrix = decay_rate * old[...] + gram[...] + ridge * identity
    square_sum = jnp.sum(jnp.sum(matrix * matrix, axis=0, keepdims=True), axis=1, keepdims=True)
    inv_norm = lax.rsqrt(square_sum)
    scaled = matrix * inv_norm
    gram[...] = scaled
    root[...] = jnp.sqrt(jnp.sqrt(inv_norm)) * (1.25 * identity - 0.25 * scaled)

    def one_turn(_, carry):
        m = gram[...]
        mb = m.astype(BF)
        q = ((dot(mb, mb) - 10.0 * m) * 0.0625).astype(BF)
        t = 1.5625 * m + dot(q, mb)
        m = 1.5625 * t + dot(q, t.astype(BF))
        gram[...] = m
        x = root[...]
        root[...] = 1.25 * x - 0.25 * dot(x.astype(BF), m.astype(BF))
        return carry

    lax.fori_loop(1, turns, one_turn, 0)
    new_root[...] = root[...].astype(BF)

    fetches[4].wait()
    kept = dot(cotan_t[...], acts[1]).astype(BF)
    gram_into(kept, kept_odd, gram)
    fetches[5].wait()
    new_stats[...] = decay_rate * stats[...] + gram[...]


def from_partner(x, partner):
    count = lax.axis_size("group")
    return lax.ppermute(x, "group", [(partner(i), i) for i in range(count)])


def stepped(i, step):
    z, y = i // SIDE, i % SIDE
    return (z + step[0]) % SIDE * SIDE + (y + step[1]) % SIDE


def pair(i):
    return i ^ 1


def per_device(acts, cotan, stats, roots, owner, task_of, counts):
    groups = lax.axis_size("group")
    rows = lax.axis_size("dp")
    position = lax.axis_index("group")
    n = stats.shape[-1]
    half = position % 2
    my_task = task_of[position]
    old_stats = stats[0, 0]
    own_root = roots[0, 0]

    strips = pl.pallas_call(
        pack_kernel,
        out_shape=jax.ShapeDtypeStruct((groups, STRIP, LANES), BF),
        in_specs=vmem(2),
        out_specs=vmem(1)[0],
        name="pack_strips",
    )(old_stats, acts)
    middle = lax.all_to_all(strips, "group", split_axis=0, concat_axis=0, tiled=True)
    first_part = (position // SIDE + 3 * (position % SIDE)) % PARTS
    other_acts = from_partner(acts, pair)
    other_root = from_partner(own_root, pair)
    scalars = jnp.stack([half, counts[position], my_task % 2, first_part])
    middle, other_acts, other_root, scalars = lax.optimization_barrier(
        (middle, other_acts, other_root, scalars)
    )
    chosen_stats, chosen_acts = pl.pallas_call(
        select_kernel,
        out_shape=(
            jax.ShapeDtypeStruct((groups, STAT_ROWS, LANES), BF),
            jax.ShapeDtypeStruct((groups, STRIP - STAT_ROWS, LANES), BF),
        ),
        in_specs=[smem(), smem()] + vmem(1),
        out_specs=tuple(vmem(2)),
        name="select_strips",
    )(owner, task_of // 2 * 2 + half, middle)
    arrived_acts = lax.all_to_all(chosen_acts, "group", split_axis=0, concat_axis=0, tiled=True)

    both_acts = pl.pallas_call(
        acts_kernel,
        out_shape=jax.ShapeDtypeStruct((acts.shape[0], 2 * n), BF),
        in_specs=[smem()] + vmem(3),
        out_specs=vmem(1)[0],
        name="join_acts",
    )(jnp.reshape(half, (1,)), acts, other_acts, arrived_acts)
    both_acts, chosen_stats = lax.optimization_barrier((both_acts, chosen_stats))
    all_acts = lax.all_gather(both_acts, "dp", axis=0, tiled=True)
    arrived = lax.all_to_all(chosen_stats, "group", split_axis=0, concat_axis=0, tiled=True)

    tokens = cotan.shape[0]
    depth = n // PARTS
    piece = pl.pallas_call(
        cotan_kernel,
        out_shape=jax.ShapeDtypeStruct((rows * depth, tokens), BF),
        in_specs=[smem(), pl.BlockSpec(memory_space=pl.ANY)],
        out_specs=vmem(1)[0],
        scratch_shapes=[pltpu.VMEM((rows, tokens, LANES), BF), pltpu.SemaphoreType.DMA((rows,))],
        name="cotan_part",
    )(jnp.reshape(first_part, (1,)), cotan)
    pieces = lax.all_gather(piece, "dp", axis=0)
    part = lax.dynamic_slice_in_dim(pieces, lax.axis_index("dp") * depth, depth, 1)
    parts = [part] + [from_partner(part, lambda i, step=step: stepped(i, step)) for step in STEPS]

    update, new_stats, new_root = pl.pallas_call(
        step_kernel,
        out_shape=(
            jax.ShapeDtypeStruct((n, n // 2), BF),
            jax.ShapeDtypeStruct((n, n), F32),
            jax.ShapeDtypeStruct((n, n), BF),
        ),
        in_specs=[smem()] + vmem(PARTS) + [pl.BlockSpec(memory_space=pl.ANY)] * 5,
        out_specs=tuple(vmem(3)),
        scratch_shapes=[
            pltpu.VMEM((n, rows * tokens), BF),
            pltpu.VMEM((2, rows * tokens, n), BF),
            pltpu.VMEM((n, n), BF),
            pltpu.VMEM((n, n), BF),
            pltpu.VMEM(arrived.shape, BF),
            pltpu.VMEM((n, n), F32),
            pltpu.VMEM((n, n), F32),
            pltpu.VMEM((n, n), F32),
            pltpu.VMEM((n, n), F32),
            pltpu.SemaphoreType.DMA((6,)),
        ],
        name="shampoo_step",
    )(
        scalars,
        *parts,
        all_acts,
        own_root,
        other_root,
        arrived,
        old_stats,
    )
    return (update, new_stats[None, None], new_root[None, None])


def solution(mesh):
    return jax.shard_map(
        per_device,
        mesh=mesh,
        in_specs=(
            P("dp", "group"),
            P("dp", None),
            P("dp", "group", None, None),
            P("dp", "group", None, None),
            P(),
            P(),
            P(),
        ),
        out_specs=(P("dp", "group"), P("dp", "group", None, None), P("dp", "group", None, None)),
        check_vma=False,
    )
```

```python
import jax
import jax.numpy as jnp
from jax import lax
from jax.experimental import pallas as pl
from jax.experimental.pallas import tpu as pltpu
from jax.sharding import PartitionSpec as P

decay_rate = 0.9
ridge = 0.001
BF = jnp.bfloat16
F32 = jnp.float32
LANES = 128
SIDE = 8
PARTS = 8
STEPS = ((1, 0), (2, 0), (0, 1), (1, 1), (0, -1), (-2, 0), (-1, 0))
STAT_ROWS = 24
STRIP = 32


def dot(a, b, dims=((1,), (0,))):
    return lax.dot_general(a, b, (dims, ((), ())), preferred_element_type=F32)


def smem():
    return pl.BlockSpec(memory_space=pltpu.SMEM)


def vmem(count):
    return [pl.BlockSpec(memory_space=pltpu.VMEM)] * count


def strip_tiles(groups):
    half = groups // 2
    low = half * 8
    for a in range(half):
        for strip, place, row, lane in (
            (a, 0, a * 8, 0),
            (a, 1, a * 8, 1),
            (a, 2, low + a * 8, 0),
            (half + a, 0, low + a * 8, 1),
            (half + a, 1, low + a * 8, 2),
            (half + a, 2, low + a * 8, 3),
        ):
            yield strip, place * 8, row, lane * LANES


def pack_kernel(stats, acts, out):
    groups = out.shape[0]
    for strip, place, row, lane in strip_tiles(groups):
        out[strip, place : place + 8, :] = stats[row : row + 8, lane : lane + LANES].astype(BF)
    for tile in range(groups // 2):
        row, lane = tile // 2 * 8, tile % 2 * LANES
        piece = acts[row : row + 8, lane : lane + LANES]
        out[2 * tile, STAT_ROWS:, :] = piece
        out[2 * tile + 1, STAT_ROWS:, :] = piece


def select_kernel(stat_source, act_source, middle, out):
    def one(o, carry):
        out[o, :STAT_ROWS, :] = middle[stat_source[o], :STAT_ROWS, :]
        out[o, STAT_ROWS:, :] = middle[act_source[o], STAT_ROWS:, :]
        return carry

    lax.fori_loop(0, out.shape[0], one, 0, unroll=8)


def acts_kernel(scalars, own, other, arrived, out):
    cols = own.shape[1]
    half = scalars[0]

    @pl.when(half == 0)
    def _():
        out[:, :cols] = own[...]
        out[:, cols : 2 * cols] = other[...]

    @pl.when(half == 1)
    def _():
        out[:, :cols] = other[...]
        out[:, cols : 2 * cols] = own[...]

    for strip in range(arrived.shape[0]):
        tile, side = strip // 2, strip % 2
        row, lane = tile // 2 * 8, 2 * cols + side * cols + tile % 2 * LANES
        out[row : row + 8, lane : lane + LANES] = arrived[strip, STAT_ROWS:, :]


def cotan_kernel(scalars, cotan, out, buffer, sems):
    count = buffer.shape[0]
    depth = out.shape[0] // count
    fold = LANES // depth
    part = scalars[0]

    def copy(k):
        start = pl.multiple_of((k * (PARTS // fold) + part // fold) * LANES, LANES)
        return pltpu.make_async_copy(cotan.at[:, pl.ds(start, LANES)], buffer.at[k], sems.at[k])

    for k in range(count):
        copy(k).start()
    for k in range(count):
        copy(k).wait()
    for side in range(fold):

        @pl.when(part % fold == side)
        def _():
            for k in range(count):
                turned = buffer[k].T
                out[k * depth : (k + 1) * depth, :] = turned[side * depth : (side + 1) * depth, :]


def gram_into(block, odd, out_ref):
    @pl.when(odd == 0)
    def _():
        out_ref[...] = dot(block, block, ((1,), (1,)))

    @pl.when(odd == 1)
    def _():
        out_ref[...] = dot(block, block, ((0,), (0,)))


def step_kernel(scalars, *refs):
    parts, refs = refs[:PARTS], refs[PARTS:]
    acts_in, own_root_in, other_root_in, arrived_in, stats_in, *refs = refs
    update, new_stats, new_root, *refs = refs
    cotan_t, acts, own_root, other_root, arrived, stats, gram, old, root, sems = refs
    half = scalars[0]
    turns = scalars[1]
    kept_odd = scalars[2]
    first_part = scalars[3]
    n = stats.shape[0]
    half_cols = n // 2
    depth = n // PARTS

    fetches = [
        pltpu.make_async_copy(source, target, sems.at[index])
        for index, (source, target) in enumerate(
            (
                (arrived_in, arrived),
                (acts_in.at[:, :n], acts.at[0]),
                (own_root_in, own_root),
                (other_root_in, other_root),
                (acts_in.at[:, n:], acts.at[1]),
                (stats_in, stats),
            )
        )
    ]
    for fetch in fetches:
        fetch.start()

    for shift, part in enumerate(parts):
        start = pl.multiple_of((first_part + shift) % PARTS * depth, depth)
        for i in range(part.shape[0]):
            cotan_t[pl.ds(start, depth), i * LANES : (i + 1) * LANES] = part[i]

    fetches[0].wait()
    for strip, place, row, lane in strip_tiles(arrived.shape[0]):
        old[row : row + 8, lane : lane + LANES] = arrived[strip, place : place + 8, :].astype(F32)
    old[:half_cols, half_cols:] = old[half_cols:, :half_cols].T

    fetches[1].wait()
    own = dot(cotan_t[...], acts[0]).astype(BF)
    fetches[2].wait()
    fetches[3].wait()

    @pl.when(half == 0)
    def _():
        left_part = dot(own_root[...], own).astype(BF)
        update[...] = dot(left_part, other_root[:, :half_cols]).astype(BF)

    @pl.when(half == 1)
    def _():
        left_part = dot(other_root[...], own).astype(BF)
        update[...] = dot(left_part, own_root[:, half_cols:]).astype(BF)

    gram_into(own, half, gram)
    identity = (
        lax.broadcasted_iota(jnp.int32, (n, n), 0) == lax.broadcasted_iota(jnp.int32, (n, n), 1)
    ).astype(F32)
    matrix = decay_rate * old[...] + gram[...] + ridge * identity
    square_sum = jnp.sum(jnp.sum(matrix * matrix, axis=0, keepdims=True), axis=1, keepdims=True)
    inv_norm = lax.rsqrt(square_sum)
    scaled = matrix * inv_norm
    gram[...] = scaled
    root[...] = jnp.sqrt(jnp.sqrt(inv_norm)) * (1.25 * identity - 0.25 * scaled)

    def one_turn(_, carry):
        m = gram[...]
        mb = m.astype(BF)
        q = ((dot(mb, mb) - 10.0 * m) * 0.0625).astype(BF)
        t = 1.5625 * m + dot(q, mb)
        m = 1.5625 * t + dot(q, t.astype(BF))
        gram[...] = m
        x = root[...]
        root[...] = 1.25 * x - 0.25 * dot(x.astype(BF), m.astype(BF))
        return carry

    lax.fori_loop(1, turns, one_turn, 0)
    new_root[...] = root[...].astype(BF)

    fetches[4].wait()
    kept = dot(cotan_t[...], acts[1]).astype(BF)
    gram_into(kept, kept_odd, gram)
    fetches[5].wait()
    new_stats[...] = decay_rate * stats[...] + gram[...]


def from_partner(x, partner):
    count = lax.axis_size("group")
    return lax.ppermute(x, "group", [(partner(i), i) for i in range(count)])


def stepped(i, step):
    z, y = i // SIDE, i % SIDE
    return (z + step[0]) % SIDE * SIDE + (y + step[1]) % SIDE


def pair(i):
    return i ^ 1


def per_device(acts, cotan, stats, roots, owner, task_of, counts):
    groups = lax.axis_size("group")
    rows = lax.axis_size("dp")
    position = lax.axis_index("group")
    n = stats.shape[-1]
    half = position % 2
    my_task = task_of[position]
    old_stats = stats[0, 0]
    own_root = roots[0, 0]

    strips = pl.pallas_call(
        pack_kernel,
        out_shape=jax.ShapeDtypeStruct((groups, STRIP, LANES), BF),
        in_specs=vmem(2),
        out_specs=vmem(1)[0],
        name="pack_strips",
    )(old_stats, acts)
    middle = lax.all_to_all(strips, "group", split_axis=0, concat_axis=0, tiled=True)
    first_part = (position // SIDE + 3 * (position % SIDE)) % PARTS
    other_acts = from_partner(acts, pair)
    scalars = jnp.stack([half, counts[position], my_task % 2, first_part])
    middle, other_acts, scalars = lax.optimization_barrier((middle, other_acts, scalars))
    chosen = pl.pallas_call(
        select_kernel,
        out_shape=jax.ShapeDtypeStruct((groups, STRIP, LANES), BF),
        in_specs=[smem(), smem()] + vmem(1),
        out_specs=vmem(1)[0],
        name="select_strips",
    )(owner, task_of // 2 * 2 + half, middle)
    arrived = lax.all_to_all(chosen, "group", split_axis=0, concat_axis=0, tiled=True)

    both_acts = pl.pallas_call(
        acts_kernel,
        out_shape=jax.ShapeDtypeStruct((acts.shape[0], 2 * n), BF),
        in_specs=[smem()] + vmem(3),
        out_specs=vmem(1)[0],
        name="join_acts",
    )(jnp.reshape(half, (1,)), acts, other_acts, arrived)
    all_acts = lax.all_gather(both_acts, "dp", axis=0, tiled=True)

    tokens = cotan.shape[0]
    depth = n // PARTS
    piece = pl.pallas_call(
        cotan_kernel,
        out_shape=jax.ShapeDtypeStruct((rows * depth, tokens), BF),
        in_specs=[smem(), pl.BlockSpec(memory_space=pl.ANY)],
        out_specs=vmem(1)[0],
        scratch_shapes=[pltpu.VMEM((rows, tokens, LANES), BF), pltpu.SemaphoreType.DMA((rows,))],
        name="cotan_part",
    )(jnp.reshape(first_part, (1,)), cotan)
    pieces = lax.all_gather(piece, "dp", axis=0)
    part = lax.dynamic_slice_in_dim(pieces, lax.axis_index("dp") * depth, depth, 1)
    parts = [part] + [from_partner(part, lambda i, step=step: stepped(i, step)) for step in STEPS]

    other_root = from_partner(own_root, pair)

    update, new_stats, new_root = pl.pallas_call(
        step_kernel,
        out_shape=(
            jax.ShapeDtypeStruct((n, n // 2), BF),
            jax.ShapeDtypeStruct((n, n), F32),
            jax.ShapeDtypeStruct((n, n), BF),
        ),
        in_specs=[smem()] + vmem(PARTS) + [pl.BlockSpec(memory_space=pl.ANY)] * 5,
        out_specs=tuple(vmem(3)),
        scratch_shapes=[
            pltpu.VMEM((n, rows * tokens), BF),
            pltpu.VMEM((2, rows * tokens, n), BF),
            pltpu.VMEM((n, n), BF),
            pltpu.VMEM((n, n), BF),
            pltpu.VMEM(arrived.shape, BF),
            pltpu.VMEM((n, n), F32),
            pltpu.VMEM((n, n), F32),
            pltpu.VMEM((n, n), F32),
            pltpu.VMEM((n, n), F32),
            pltpu.SemaphoreType.DMA((6,)),
        ],
        name="shampoo_step",
    )(
        scalars,
        *parts,
        all_acts,
        own_root,
        other_root,
        arrived,
        old_stats,
    )
    return (update, new_stats[None, None], new_root[None, None])


def solution(mesh):
    return jax.shard_map(
        per_device,
        mesh=mesh,
        in_specs=(
            P("dp", "group"),
            P("dp", None),
            P("dp", "group", None, None),
            P("dp", "group", None, None),
            P(),
            P(),
            P(),
        ),
        out_specs=(P("dp", "group"), P("dp", "group", None, None), P("dp", "group", None, None)),
        check_vma=False,
    )
```
